32 devices in a mesh: rep: 2 (over y), seq: 4 (over z), head: 2 (over x), sub: 2 (over core).
Axes of the slice: x: 2, y: 2, z: 4, core: 2. Of those that a mesh axis runs over, the one named last changes fastest.
Arguments:
- tokens: bfloat16 [32, 4096], P(('rep', 'sub'), 'seq'), parts along dimension 0, may hold values from -260 to 260
- attn_gain: float32 [4096], P('seq'), may hold values from 0.1 to 1.9
- w_query: bfloat16 [4096, 4096], P('seq', 'head'), may hold values from -0.09375 to 0.09375
- key_projection_weight: bfloat16 [4096, 1024], P('seq', 'head'), may hold values from -0.375 to 0.375
- value_projection_weight: bfloat16 [4096, 1024], P('seq', 'head'), may hold values from -0.375 to 0.375
- w_attn_out: bfloat16 [4096, 4096], P('head', 'seq'), may hold values from -0.09375 to 0.09375
- cache_keys: bfloat16 [32, 8, 2048, 128], P(('rep', 'sub'), 'head', 'seq'), parts along dimension 0, may hold values from -2500 to 2500
- stored_value_cache: bfloat16 [32, 8, 2048, 128], P(('rep', 'sub'), 'head', 'seq'), parts along dimension 0, may hold values from -12 to 12
- lengths: int32 [32], P(('rep', 'sub')), parts along dimension 0, may hold values from 1024 to 2048
- positions: int32 [32], P(('rep', 'sub')), parts along dimension 0, may hold values from 0 to 2047
- mamba_gain: float32 [4096], replicated, may hold values from 0.1 to 1.9
- w_in: bfloat16 [2, 4096, 8192], P(None, None, ('seq', 'head')), may hold values from -0.09375 to 0.09375
- conv_weight: float32 [4, 8192], P(None, ('seq', 'head')), may hold values from -3 to 3
- conv_bias: float32 [8192], P(('seq', 'head')), may hold values from -0.5 to 0.5
- conv_state: float32 [32, 3, 8192], P(('rep', 'sub'), None, ('seq', 'head')), parts along dimension 0, may hold values from -6 to 6
- w_xproj: bfloat16 [8192, 288], P(('seq', 'head')), may hold values from -0.0625 to 0.0625
- w_dt: bfloat16 [256, 8192], P(None, ('seq', 'head')), may hold values from -0.375 to 0.375
- dt_bias: float32 [8192], P(('seq', 'head')), may hold values from -4 to 0
- a_log: float32 [16, 8192], P(None, ('seq', 'head')), may hold values from 0 to 2.77
- skip_gain: float32 [8192], P(('seq', 'head')), may hold values from 0.25 to 2
- ssm_state: float32 [32, 16, 8192], P(('rep', 'sub'), None, ('seq', 'head')), parts along dimension 0, may hold values from -6 to 6
- w_mamba_out: bfloat16 [8192, 4096], P(('seq', 'head')), may hold values from -0.09375 to 0.09375
Outputs:
- hidden_out: bfloat16 [32, 4096], P(('rep', 'sub'), 'seq'), parts along dimension 0
- new_state: float32 [32, 16, 8192], P(('rep', 'sub'), None, ('seq', 'head')), parts along dimension 0
The draws below stay inside these ranges and needn't reach their ends.
There are 2 independent parts, one for each index of `rep`. The reference program is written for one: setup_inputs(seed, part) draws one part's arguments, and reference() takes and returns one part's arrays. A program takes and returns all parts, laid end to end along the dimension named above; an argument that names none is the same for every part. Nothing has to cross between parts.
Inputs may be any that keep to these rules, and one draw needn't show every extreme that they name: Cache positions p < lengths[b] hold sequence b's past keys and values; later positions are not attended.
All inputs are finite; a program needn't handle non-finite values.
Results may differ from the reference program's by a relative error of at most 0.015.
Values may be sent and summed in bfloat16 or wider, within the bound.
A program may use at most 128 MiB of HBM per device.

```python
import math
import jax
import jax.numpy as jnp
from jax import lax

MODEL_DIMENSION = 4096
QUERY_HEADS = 32
KEY_VALUE_HEADS = 8
HEAD_SIZE = 128
DI = 8192
NSTATE = 16
DT_RANK = 256
KCONV = 4
BATCH_SEQUENCES = 16
CACHE_POSITIONS = 2048


def draw_tokens(key, part):
    base_key_rows = jax.random.fold_in(jax.random.fold_in(key, 11), 0)
    base_draw = jnp.clip(jax.random.normal(base_key_rows, (BATCH_SEQUENCES, MODEL_DIMENSION), jnp.float32), -6.0, 6.0)
    across = jnp.arange(MODEL_DIMENSION, dtype=jnp.float32) / MODEL_DIMENSION
    value_vectors = base_draw * jnp.sqrt(1.0 + 2.0 * across)[None, :]
    return value_vectors.astype(jnp.bfloat16)


def draw_cache_keys(key, part):
    base_key_rows = jax.random.fold_in(jax.random.fold_in(key, 23), 0)
    value_vectors = 2.5 * jnp.clip(jax.random.normal(base_key_rows, (BATCH_SEQUENCES, KEY_VALUE_HEADS, CACHE_POSITIONS, HEAD_SIZE), jnp.float32), -6.0, 6.0)
    return value_vectors.astype(jnp.bfloat16)


def draw_stored_value_cache(key, part):
    noise_key, common_key = jax.random.split(jax.random.fold_in(key, 37), 2)
    shape = (BATCH_SEQUENCES, KEY_VALUE_HEADS, CACHE_POSITIONS, HEAD_SIZE)
    common = jnp.clip(jax.random.normal(common_key, (BATCH_SEQUENCES, KEY_VALUE_HEADS, 1, HEAD_SIZE), jnp.float32), -4.0, 4.0)
    along = (jnp.arange(CACHE_POSITIONS, dtype=jnp.float32) / CACHE_POSITIONS)[None, None, :, None]
    noise = jnp.clip(jax.random.normal(noise_key, shape, jnp.float32), -6.0, 6.0)
    ramp = 0.3 + 0.7 * along
    return (noise + ramp * common).astype(jnp.bfloat16)


def set_ends(result, own_key, least, largest):
    dims = result.shape
    spot = [jax.random.randint(jax.random.fold_in(own_key, axis), (), 0, dims[axis]) for axis in range(len(dims))]
    result = result.at[tuple(spot)].set(least)
    longest = dims.index(max(dims))
    spot[longest] = (spot[longest] + 1) % dims[longest]
    return result.at[tuple(spot)].set(largest)


def raised(result, stream_key, source, target, shards_of, factor):
    owner, partner = [(jnp.arange(result.shape[dim]) // (result.shape[dim] // shards_of)).reshape([-1 if axis == dim else 1 for axis in range(result.ndim)]) for dim in (source, target)]
    chosen = jax.random.permutation(stream_key, shards_of)[partner]
    strong = (owner == chosen) | (owner == (partner + shards_of // 2) % shards_of)
    return jnp.where(strong, factor * result, result)


def shard_levels(stream_key, dims, shards, least, largest):
    level = 1.0
    for dim, blocks in shards:
        heights = jax.random.uniform(jax.random.fold_in(jax.random.fold_in(stream_key, 6), dim), (blocks,), jnp.float32, least / len(shards), largest / len(shards))
        level = level * jnp.repeat(jnp.exp(heights), dims[dim] // blocks).reshape((-1,) + (1,) * (len(dims) - 1 - dim))
    return level


def normal_values(own_key, extent, deviation, reach, pieces=(), held_as=jnp.bfloat16):
    array = deviation * jax.random.normal(own_key, extent, jnp.float32)
    if pieces:
        array = array * shard_levels(own_key, extent, pieces, -0.22, 0.18)
    return jnp.clip(array, -reach, reach).astype(held_as)


def bell_draw_with(own_key, shape, spread, most, pieces, heavy, kind=jnp.bfloat16):
    drawn = spread * jax.random.normal(own_key, shape, jnp.float32)
    if pieces:
        drawn = drawn * shard_levels(own_key, shape, pieces, -0.22, 0.18)
    return jnp.clip(raised(drawn, jax.random.fold_in(own_key, 3), *heavy), -most, most).astype(kind)


def setup_inputs(seed: int = 0, part: int = 0) -> dict:
    keys = jax.random.split(jax.random.key(seed), 23)
    own_keys = jax.random.split(jax.random.fold_in(keys[22], part), 23)
    tokens = draw_tokens(jax.random.fold_in(jax.random.fold_in(keys[22], part), 71), part)
    attn_gain = jnp.clip(1.0 + 0.18 * jax.random.normal(keys[1], (MODEL_DIMENSION,), jnp.float32), 0.1, 1.9)
    w_query = normal_values(keys[2], (MODEL_DIMENSION, QUERY_HEADS * HEAD_SIZE), MODEL_DIMENSION ** -0.5, 0.09375, ((0, 4), (1, 2)))
    key_projection_weight = normal_values(keys[3], (MODEL_DIMENSION, KEY_VALUE_HEADS * HEAD_SIZE), (MODEL_DIMENSION // 16) ** -0.5, 0.375, ((0, 4), (1, 2)))
    value_projection_weight = normal_values(keys[4], (MODEL_DIMENSION, KEY_VALUE_HEADS * HEAD_SIZE), (MODEL_DIMENSION // 16) ** -0.5, 0.375, ((0, 4), (1, 2)))
    w_attn_out = normal_values(keys[5], (QUERY_HEADS * HEAD_SIZE, MODEL_DIMENSION), (QUERY_HEADS * HEAD_SIZE) ** -0.5, 0.09375, ((0, 2), (1, 4)))
    cache_keys = draw_cache_keys(jax.random.fold_in(jax.random.fold_in(keys[22], part), 71), part)
    stored_value_cache = draw_stored_value_cache(jax.random.fold_in(jax.random.fold_in(keys[22], part), 71), part)
    lengths = set_ends(jax.random.randint(own_keys[8], (BATCH_SEQUENCES,), CACHE_POSITIONS // 2, CACHE_POSITIONS + 1), jax.random.fold_in(own_keys[8], 1), CACHE_POSITIONS // 2, CACHE_POSITIONS).astype(jnp.int32)
    positions = set_ends(jax.random.randint(own_keys[9], (BATCH_SEQUENCES,), 0, CACHE_POSITIONS), jax.random.fold_in(own_keys[9], 1), 0, CACHE_POSITIONS - 1).astype(jnp.int32)
    mamba_gain = jnp.clip(1.0 + 0.18 * jax.random.normal(keys[10], (MODEL_DIMENSION,), jnp.float32), 0.1, 1.9)
    w_in = normal_values(keys[11], (2, MODEL_DIMENSION, DI), MODEL_DIMENSION ** -0.5, 0.09375, ((2, 8),))
    conv_weight = normal_values(keys[12], (KCONV, DI), KCONV ** -0.5, 3.0, ((1, 8),), jnp.float32)
    conv_bias = jnp.clip(jax.random.uniform(keys[13], (DI,), jnp.float32, -0.5, 0.5) * shard_levels(keys[13], (DI,), ((0, 8),), -0.4, 0.0), -0.5, 0.5)
    conv_state = normal_values(own_keys[14], (BATCH_SEQUENCES, KCONV - 1, DI), 1.0, 6.0, ((0, 2), (2, 8)), jnp.float32)
    w_xproj = normal_values(keys[15], (DI, DT_RANK + 2 * NSTATE), DI ** -0.5, 0.0625, ((0, 8),))
    w_dt = normal_values(keys[16], (DT_RANK, DI), DT_RANK ** -0.5, 0.375, ((1, 8),))
    dt_bias = jnp.clip(-4.0 + 4.0 * jax.random.uniform(keys[17], (DI,), jnp.float32) ** shard_levels(keys[17], (DI,), ((0, 8),), -0.2, 0.2), -4.0, 0.0)
    a_log = jnp.clip(2.77 * jax.random.uniform(keys[18], (NSTATE, DI), jnp.float32) ** shard_levels(keys[18], (NSTATE, DI), ((1, 8),), -0.2, 0.2), 0.0, 2.77)
    skip_gain = jnp.clip(0.25 + 1.75 * jax.random.uniform(keys[19], (DI,), jnp.float32) ** shard_levels(keys[19], (DI,), ((0, 8),), -0.2, 0.2), 0.25, 2.0)
    ssm_state = normal_values(own_keys[20], (BATCH_SEQUENCES, NSTATE, DI), 1.0, 6.0, ((0, 2), (2, 8)), jnp.float32)
    w_mamba_out = bell_draw_with(keys[21], (DI, MODEL_DIMENSION), DI ** -0.5, 0.09375, ((0, 8),), (0, 1, 8, 2.0))
    return {"tokens": tokens, "attn_gain": attn_gain, "w_query": w_query, "key_projection_weight": key_projection_weight, "value_projection_weight": value_projection_weight, "w_attn_out": w_attn_out, "cache_keys": cache_keys, "stored_value_cache": stored_value_cache, "lengths": lengths, "positions": positions, "mamba_gain": mamba_gain, "w_in": w_in, "conv_weight": conv_weight, "conv_bias": conv_bias, "conv_state": conv_state, "w_xproj": w_xproj, "w_dt": w_dt, "dt_bias": dt_bias, "a_log": a_log, "skip_gain": skip_gain, "ssm_state": ssm_state, "w_mamba_out": w_mamba_out}


norm_eps = 1e-05
rope_base = 10000.0

def apply_rotary(vectors, positions):
    half_dim = vectors.shape[-1] // 2
    frequency = jnp.exp(-math.log(rope_base) * 2.0 * jnp.arange(half_dim, dtype=jnp.float32) / (2 * half_dim))
    angles = positions.astype(jnp.float32)[:, None] * frequency[None, :]
    cosine = jnp.cos(angles)[:, None, :]
    sine_part = jnp.sin(angles)[:, None, :]
    first_half = vectors[..., :half_dim]
    second_half = vectors[..., half_dim:]
    return jnp.concatenate([first_half * cosine - second_half * sine_part, second_half * cosine + first_half * sine_part], axis=-1)

def reference(tokens, attn_gain, w_query, key_projection_weight, value_projection_weight, w_attn_out, cache_keys, stored_value_cache, lengths, positions, mamba_gain, w_in, conv_weight, conv_bias, conv_state, w_xproj, w_dt, dt_bias, a_log, skip_gain, ssm_state, w_mamba_out):
    token_float = tokens.astype(jnp.float32)
    inv_rms = lax.rsqrt(lax.optimization_barrier(jnp.sum(token_float * token_float, axis=1)) / MODEL_DIMENSION + norm_eps)
    lifted = (token_float * attn_gain[None, :]).astype(jnp.bfloat16)
    query_vectors = jnp.dot(lifted, w_query, preferred_element_type=jnp.float32) * inv_rms[:, None]
    fresh_key_rows = jnp.dot(lifted, key_projection_weight, preferred_element_type=jnp.float32) * inv_rms[:, None]
    fresh_value_rows = jnp.dot(lifted, value_projection_weight, preferred_element_type=jnp.float32) * inv_rms[:, None]
    query_vectors = apply_rotary(query_vectors.reshape(BATCH_SEQUENCES, QUERY_HEADS, HEAD_SIZE), positions).astype(jnp.bfloat16)
    fresh_key_rows = apply_rotary(fresh_key_rows.reshape(BATCH_SEQUENCES, KEY_VALUE_HEADS, HEAD_SIZE), positions).astype(jnp.bfloat16)
    fresh_value_rows = fresh_value_rows.reshape(BATCH_SEQUENCES, KEY_VALUE_HEADS, HEAD_SIZE).astype(jnp.bfloat16)
    query_group_count = QUERY_HEADS // KEY_VALUE_HEADS
    grouped_queries = query_vectors.reshape(BATCH_SEQUENCES, KEY_VALUE_HEADS, query_group_count, HEAD_SIZE).astype(jnp.float32)
    score_scale = HEAD_SIZE ** (-0.5)
    scores = jnp.einsum('bhgd,bhtd->bhgt', grouped_queries, cache_keys.astype(jnp.float32)) * score_scale
    score_new = jnp.einsum('bhgd,bhd->bhg', grouped_queries, fresh_key_rows.astype(jnp.float32)) * score_scale
    live_mask = jnp.arange(CACHE_POSITIONS, dtype=jnp.int32)[None, None, None, :] < lengths[:, None, None, None]
    row_max = jnp.maximum(lax.optimization_barrier(jnp.max(jnp.where(live_mask, scores, -jnp.inf), axis=-1)), score_new)
    weights = jnp.where(live_mask, jnp.exp(scores - row_max[..., None]), 0.0)
    new_weight = jnp.exp(score_new - row_max)
    total_weight = lax.optimization_barrier(jnp.sum(weights, axis=-1)) + new_weight
    rounded = lax.optimization_barrier(weights.astype(jnp.bfloat16)).astype(jnp.float32)
    attended = jnp.einsum('bhgt,bhtd->bhgd', rounded, stored_value_cache.astype(jnp.float32))
    attended = attended + new_weight[..., None] * fresh_value_rows.astype(jnp.float32)[:, :, None, :]
    attn_rows = (attended / total_weight[..., None]).reshape(BATCH_SEQUENCES, QUERY_HEADS * HEAD_SIZE).astype(jnp.bfloat16)
    mid_stream = (token_float + jnp.dot(attn_rows, w_attn_out, preferred_element_type=jnp.float32)).astype(jnp.bfloat16)
    mid_float = mid_stream.astype(jnp.float32)
    inv_rms_two = lax.rsqrt(lax.optimization_barrier(jnp.mean(mid_float * mid_float, axis=1)) + norm_eps)
    lifted_two = (mid_float * inv_rms_two[:, None] * mamba_gain[None, :]).astype(jnp.bfloat16)
    inner = jnp.dot(lifted_two, w_in[0], preferred_element_type=jnp.float32)
    gate_branch = jnp.dot(lifted_two, w_in[1], preferred_element_type=jnp.float32)
    window = jnp.concatenate([conv_state, inner[:, None, :]], axis=1)
    mixed = lax.optimization_barrier(jnp.sum(window * conv_weight[None, :, :], axis=1)) + conv_bias[None, :]
    activated = jax.nn.silu(mixed)
    projected = jnp.dot(activated.astype(jnp.bfloat16), w_xproj, preferred_element_type=jnp.float32)
    dt_low = projected[:, :DT_RANK].astype(jnp.bfloat16)
    input_map = projected[:, DT_RANK:DT_RANK + NSTATE]
    output_map = projected[:, DT_RANK + NSTATE:]
    step_size = jax.nn.softplus(jnp.dot(dt_low, w_dt, preferred_element_type=jnp.float32) + dt_bias[None, :])
    decay = jnp.exp(step_size[:, None, :] * (-jnp.exp(a_log))[None, :, :])
    new_state = decay * ssm_state + (step_size * activated)[:, None, :] * input_map[:, :, None]
    readout = lax.optimization_barrier(jnp.sum(output_map[:, :, None] * new_state, axis=1)) + skip_gain[None, :] * activated
    gated = (readout * jax.nn.silu(gate_branch)).astype(jnp.bfloat16)
    hidden_out = (mid_float + jnp.dot(gated, w_mamba_out, preferred_element_type=jnp.float32)).astype(jnp.bfloat16)
    return (hidden_out, new_state)
```

```python
import functools
import math

import jax
import jax.numpy as jnp
from jax import lax
from jax.experimental import pallas as pl
from jax.experimental.pallas import tpu as pltpu
from jax.sharding import PartitionSpec as P

norm_eps = 1e-05
masked_floor = -1e30
rope_base = 10000.0


def joined(value, axis, join):
    pieces = jax.tree.map(lambda part: lax.all_gather(part, axis), value)
    head = jax.tree.map(lambda part: part[0], pieces)
    tail = jax.tree.map(lambda part: part[1:], pieces)
    subtotal, _ = lax.scan(lambda subtotal, section: (join(subtotal, section), None), head, tail)
    return subtotal


def apply_rotary(vectors, positions):
    half_dim = vectors.shape[-1] // 2
    frequency = jnp.exp(
        -math.log(rope_base) * 2.0 * jnp.arange(half_dim, dtype=jnp.float32) / (2 * half_dim)
    )
    angles = positions.astype(jnp.float32)[:, None] * frequency[None, :]
    cosine = jnp.cos(angles)[:, None, :]
    sine_part = jnp.sin(angles)[:, None, :]
    first_half = vectors[..., :half_dim]
    second_half = vectors[..., half_dim:]
    return jnp.concatenate(
        [
            first_half * cosine - second_half * sine_part,
            second_half * cosine + first_half * sine_part,
        ],
        axis=-1,
    )


def join_partial(earlier, later):
    max_one, sum_one, acc_one = earlier
    max_two, sum_two, acc_two = later
    joined_max = jnp.maximum(max_one, max_two)
    factor_one = jnp.exp(max_one - joined_max)
    factor_two = jnp.exp(max_two - joined_max)
    return (
        joined_max,
        sum_one * factor_one + sum_two * factor_two,
        acc_one * factor_one[..., None] + acc_two * factor_two[..., None],
    )


def local(
    tokens,
    attn_gain,
    w_query,
    key_projection_weight,
    value_projection_weight,
    w_attn_out,
    cache_keys,
    stored_value_cache,
    lengths,
    positions,
    mamba_gain,
    w_in,
    conv_weight,
    conv_bias,
    conv_state,
    w_xproj,
    w_dt,
    dt_bias,
    a_log,
    skip_gain,
    ssm_state,
    w_mamba_out,
):
    batch_rows = tokens.shape[0]
    feature_cols = tokens.shape[1]
    head_dim = cache_keys.shape[3]
    kv_local = cache_keys.shape[1]
    ctx_local = cache_keys.shape[2]
    q_local = w_query.shape[1] // head_dim
    query_group_count = q_local // kv_local
    model_width = feature_cols * lax.axis_size("seq")
    token_float = tokens.astype(jnp.float32)
    lifted = (token_float * attn_gain[None, :]).astype(jnp.bfloat16)
    part_query = jnp.dot(lifted, w_query, preferred_element_type=jnp.float32)
    part_key = jnp.dot(lifted, key_projection_weight, preferred_element_type=jnp.float32)
    part_value = jnp.dot(lifted, value_projection_weight, preferred_element_type=jnp.float32)
    squares = jnp.sum(token_float * token_float, axis=1)
    sum_squares = lax.psum(squares, "seq")
    part_query, part_key, part_value = lax.psum((part_query, part_key, part_value), "seq")
    inv_rms = lax.rsqrt(sum_squares / model_width + norm_eps)
    query_vectors = apply_rotary(
        (part_query * inv_rms[:, None]).reshape(batch_rows, q_local, head_dim), positions
    ).astype(jnp.bfloat16)
    fresh_key_rows = apply_rotary(
        (part_key * inv_rms[:, None]).reshape(batch_rows, kv_local, head_dim), positions
    ).astype(jnp.bfloat16)
    fresh_value_rows = (
        (part_value * inv_rms[:, None]).reshape(batch_rows, kv_local, head_dim).astype(jnp.bfloat16)
    )
    grouped_queries = query_vectors.reshape(batch_rows, kv_local, query_group_count, head_dim)
    score_scale = head_dim ** (-0.5)
    scores = (
        jnp.einsum(
            "bhgd,bhtd->bhgt", grouped_queries, cache_keys, preferred_element_type=jnp.float32
        )
        * score_scale
    )
    slot_index = lax.axis_index("seq") * ctx_local + jnp.arange(ctx_local, dtype=jnp.int32)
    live_mask = slot_index[None, None, None, :] < lengths[:, None, None, None]
    local_max = jnp.max(jnp.where(live_mask, scores, masked_floor), axis=-1)
    weights = jnp.where(live_mask, jnp.exp(scores - local_max[..., None]), 0.0)
    local_sum = jnp.sum(weights, axis=-1)
    local_acc = jnp.einsum(
        "bhgt,bhtd->bhgd",
        weights.astype(jnp.bfloat16),
        stored_value_cache,
        preferred_element_type=jnp.float32,
    )
    merged_max, merged_sum, merged_acc = joined(
        (local_max, local_sum, local_acc), "seq", join_partial
    )
    score_new = (
        jnp.einsum(
            "bhgd,bhd->bhg", grouped_queries.astype(jnp.float32), fresh_key_rows.astype(jnp.float32)
        )
        * score_scale
    )
    row_max = jnp.maximum(merged_max, score_new)
    old_factor = jnp.exp(merged_max - row_max)
    new_weight = jnp.exp(score_new - row_max)
    total_weight = merged_sum * old_factor + new_weight
    attended = (
        merged_acc * old_factor[..., None]
        + new_weight[..., None] * fresh_value_rows.astype(jnp.float32)[:, :, None, :]
    )
    attn_rows = (
        (attended / total_weight[..., None])
        .reshape(batch_rows, q_local * head_dim)
        .astype(jnp.bfloat16)
    )
    out_part = jnp.dot(attn_rows, w_attn_out, preferred_element_type=jnp.float32)
    summed = lax.psum(out_part, "head")
    mid_stream = (token_float + summed).astype(jnp.bfloat16)
    full_tokens = lax.all_gather(mid_stream, "seq", axis=1, tiled=True)
    full_float = full_tokens.astype(jnp.float32)
    inv_rms_two = lax.rsqrt(jnp.mean(full_float * full_float, axis=1) + norm_eps)
    lifted_two = (full_float * inv_rms_two[:, None] * mamba_gain[None, :]).astype(jnp.bfloat16)
    inner = jnp.dot(lifted_two, w_in[0], preferred_element_type=jnp.float32)
    gate_branch = jnp.dot(lifted_two, w_in[1], preferred_element_type=jnp.float32)
    window = jnp.concatenate([conv_state, inner[:, None, :]], axis=1)
    mixed = jnp.sum(window * conv_weight[None, :, :], axis=1) + conv_bias[None, :]
    activated = jax.nn.silu(mixed)
    proj_part = jnp.dot(activated.astype(jnp.bfloat16), w_xproj, preferred_element_type=jnp.float32)
    projected = lax.psum(proj_part, ("seq", "head"))
    rank_width = w_dt.shape[0]
    state_width = ssm_state.shape[1]
    dt_low = projected[:, :rank_width].astype(jnp.bfloat16)
    input_map = projected[:, rank_width : rank_width + state_width]
    output_map = projected[:, rank_width + state_width :]
    step_size = jax.nn.softplus(
        jnp.dot(dt_low, w_dt, preferred_element_type=jnp.float32) + dt_bias[None, :]
    )
    decay = jnp.exp(step_size[:, None, :] * (-jnp.exp(a_log))[None, :, :])
    new_state = decay * ssm_state + (step_size * activated)[:, None, :] * input_map[:, :, None]
    readout = jnp.sum(output_map[:, :, None] * new_state, axis=1) + skip_gain[None, :] * activated
    gated = (readout * jax.nn.silu(gate_branch)).astype(jnp.bfloat16)
    mamba_part = jnp.dot(gated, w_mamba_out, preferred_element_type=jnp.float32)
    share = lax.psum_scatter(
        mamba_part.astype(jnp.bfloat16), "seq", scatter_dimension=1, tiled=True
    ).astype(jnp.float32)
    share = lax.psum(share, "head")
    hidden_out = (mid_stream.astype(jnp.float32) + share).astype(jnp.bfloat16)
    return (hidden_out, new_state)


MESH = pl.DeviceIdType.MESH


def farthest_first(count):
    return sorted(range(1, count), key=lambda k: -min(k, count - k))


def rotate(vectors, cosine, sine_signed):
    half_dim = vectors.shape[-1] // 2
    return vectors * cosine + pltpu.roll(vectors, half_dim, 1) * sine_signed


def fused_kernel(
    seq_count,
    head_count,
    length_ref,
    position_ref,
    token_ref,
    attn_gain_ref,
    mamba_gain_ref,
    conv_weight_ref,
    conv_bias_ref,
    dt_bias_ref,
    a_log_ref,
    skip_gain_ref,
    wq_hbm,
    wk_hbm,
    wv_hbm,
    wo_hbm,
    ck_hbm,
    cv_hbm,
    win_hbm,
    cs_hbm,
    wx_hbm,
    wdt_hbm,
    state_hbm,
    wm_hbm,
    hidden_ref,
    new_state_hbm,
    wq,
    wk,
    wv,
    wo,
    ck,
    cv,
    win,
    cs,
    wx,
    wdt,
    state,
    wm,
    new_state,
    load_sem,
    q_part,
    kv_part,
    ssq_part,
    q_slots,
    kv_slots,
    ssq_slots,
    q_rows,
    scores,
    acc_rows,
    ml_rows,
    acc_part,
    ml_part,
    acc_slots,
    ml_slots,
    attn_x,
    out_part,
    out_slots,
    mid_part,
    mid_slots,
    gains,
    inner_acc,
    proj_part,
    proj_slots,
    y_rows,
    gated_x,
    share_part,
    share_slots,
    seq_send,
    seq_recv,
    head_send,
    head_recv,
    all_send,
    all_recv,
):
    rows, feature = token_ref.shape
    head_dim = ck.shape[3]
    kv_local = ck.shape[1]
    ctx = ck.shape[2]
    q_cols = wq.shape[1]
    kv_cols = wk.shape[1]
    q_heads = q_cols // head_dim
    group = q_heads // kv_local
    model = feature * seq_count
    chan = wm.shape[0]
    nstate = a_log_ref.shape[0]
    rank = wdt.shape[0]
    f32 = jnp.float32
    bf16 = jnp.bfloat16
    my_seq = lax.axis_index("seq")
    my_head = lax.axis_index("head")

    def peer(ks, kh):
        return {
            "seq": lax.rem(my_seq + ks, seq_count),
            "head": lax.rem(my_head + kh, head_count),
        }

    loads = []
    for src, dst in (
        (wq_hbm, wq),
        (wk_hbm, wk),
        (wv_hbm, wv),
        (ck_hbm, ck),
        (cv_hbm, cv),
        (wo_hbm, wo),
        (win_hbm, win),
        (cs_hbm, cs),
        (wx_hbm, wx),
        (wdt_hbm, wdt),
        (state_hbm, state),
        (wm_hbm, wm),
    ):
        copy = pltpu.make_async_copy(src, dst, load_sem.at[len(loads)])
        copy.start()
        loads.append(copy)
    (ld_wq, ld_wk, ld_wv, ld_ck, ld_cv, ld_wo, ld_win, ld_cs, ld_wx, ld_wdt, ld_state, ld_wm) = loads

    barrier = pltpu.get_barrier_semaphore()
    everyone = [
        (ks, kh) for ks in range(seq_count) for kh in range(head_count) if ks or kh
    ]
    everyone.sort(key=lambda o: -(min(o[0], seq_count - o[0]) + min(o[1], head_count - o[1])))
    for ks, kh in everyone:
        pl.semaphore_signal(barrier, inc=1, device_id=peer(ks, kh), device_id_type=MESH)

    seq_order = farthest_first(seq_count)
    near_order = seq_order[::-1]
    pending = []

    def seq_push(phase, src, slots):
        for k in seq_order:
            copy = pltpu.make_async_remote_copy(
                src_ref=src,
                dst_ref=slots.at[k],
                send_sem=seq_send.at[phase, k],
                recv_sem=seq_recv.at[phase, k],
                device_id=peer(k, 0),
                device_id_type=MESH,
            )
            copy.start()
            pending.append(copy)

    def seq_wait(phase, k, src, slots):
        pltpu.make_async_remote_copy(
            src_ref=src,
            dst_ref=slots.at[k],
            send_sem=seq_send.at[phase, k],
            recv_sem=seq_recv.at[phase, k],
            device_id=peer(k, 0),
            device_id_type=MESH,
        ).wait_recv()

    token_float = token_ref[...].astype(f32)
    lifted = (token_float * attn_gain_ref[...][None, :]).astype(bf16)
    squares = jnp.sum(token_float * token_float, axis=1, keepdims=True)
    ssq_part[...] = jnp.broadcast_to(squares, ssq_part.shape)

    half_dim = head_dim // 2
    lane = lax.broadcasted_iota(jnp.int32, (rows, head_dim), 1)
    frequency = jnp.exp(
        -math.log(rope_base) * 2.0 * (lane % half_dim).astype(f32) / (2 * half_dim)
    )
    row_index = lax.broadcasted_iota(jnp.int32, (rows, head_dim), 0)
    position = jnp.zeros((rows, head_dim), f32)
    for b in range(rows):
        position = jnp.where(row_index == b, position_ref[b].astype(f32), position)
    angles = position * frequency
    cosine = jnp.cos(angles)
    sine_signed = jnp.where(lane < half_dim, -jnp.sin(angles), jnp.sin(angles))
    mg = mamba_gain_ref[...]
    for s in range(seq_count):
        gains[s] = jnp.broadcast_to(mg[s * feature : (s + 1) * feature][None, :], (rows, feature))

    tile = 512

    def dot(a, b):
        return jnp.dot(a, b, preferred_element_type=f32)

    ld_wq.wait()
    for n in range(0, q_cols, tile):
        q_part[:, n : n + tile] = dot(lifted, wq[:, n : n + tile]).astype(bf16)
    pl.semaphore_wait(barrier, len(everyone))
    seq_push(0, ssq_part, ssq_slots)
    seq_push(1, q_part, q_slots)
    ld_wk.wait()
    kv_part[:, :kv_cols] = dot(lifted, wk[...]).astype(bf16)
    ld_wv.wait()
    kv_part[:, kv_cols:] = dot(lifted, wv[...]).astype(bf16)
    seq_push(2, kv_part, kv_slots)

    for k in near_order:
        seq_wait(0, k, ssq_part, ssq_slots)
        seq_wait(1, k, q_part, q_slots)
    ssq = ssq_part[...]
    for k in near_order:
        ssq = ssq + ssq_slots[k]
    inv_rms = lax.rsqrt(ssq / model + norm_eps)
    for j in range(q_heads):
        cols = slice(j * head_dim, (j + 1) * head_dim)
        total = q_part[:, cols].astype(f32)
        for k in near_order:
            total = total + q_slots[k, :, cols].astype(f32)
        spun = rotate(total * inv_rms, cosine, sine_signed)
        q_rows[j * rows : (j + 1) * rows, :] = spun.astype(bf16).astype(f32)

    score_scale = head_dim ** (-0.5)
    pair_rows = 2 * group
    pair_stride = pair_rows * rows
    upper = lax.broadcasted_iota(jnp.int32, (pair_rows, head_dim), 0) < group
    slot_index = my_seq * ctx + lax.broadcasted_iota(jnp.int32, (pair_rows, ctx), 1)
    pairs = [(b, p) for b in range(rows) for p in range(kv_local // 2)]
    ld_ck.wait()
    for index, (b, p) in enumerate(pairs):
        x = q_rows[pl.ds(p * pair_stride + b, pair_rows, stride=rows), :]
        left = jnp.concatenate([jnp.where(upper, x, 0.0), jnp.where(upper, 0.0, x)], axis=1)
        keys = jnp.concatenate([ck[b, 2 * p], ck[b, 2 * p + 1]], axis=1)
        scores[index] = lax.dot_general(
            left.astype(bf16), keys, (((1,), (1,)), ((), ())), preferred_element_type=f32
        )
    ld_cv.wait()
    lane_row = lax.broadcasted_iota(jnp.int32, (pair_rows, head_dim), 1)
    for index, (b, p) in enumerate(pairs):
        live = slot_index < length_ref[b]
        s = jnp.where(live, scores[index] * score_scale, masked_floor)
        top = jnp.max(s, axis=1, keepdims=True)
        w = jnp.where(live, jnp.exp(s - top), 0.0)
        sum_w = jnp.sum(w, axis=1, keepdims=True)
        values = jnp.concatenate([cv[b, 2 * p], cv[b, 2 * p + 1]], axis=1)
        both = dot(w.astype(bf16), values)
        acc = jnp.where(upper, both[:, :head_dim], both[:, head_dim:])
        acc = acc / jnp.maximum(sum_w, 1e-30)
        spot = pl.ds(p * pair_stride + b, pair_rows, stride=rows)
        acc_rows[spot, :] = acc
        ml_rows[spot, :] = jnp.where(lane_row < half_dim, top, sum_w)
    acc_part[...] = acc_rows[...].astype(bf16)
    n_rows = q_heads * rows
    diag = lax.broadcasted_iota(jnp.int32, (n_rows, n_rows), 0) == lax.broadcasted_iota(
        jnp.int32, (n_rows, n_rows), 1
    )

    def to_lanes(column):
        return jnp.sum(jnp.where(diag, column, 0.0), axis=0, keepdims=True)

    def to_rows(line):
        return jnp.sum(jnp.where(diag, line, 0.0), axis=1, keepdims=True)

    ml = ml_rows[...]
    ml_part[0:1, :] = to_lanes(ml[:, 0:1])
    ml_part[1:2, :] = to_lanes(ml[:, half_dim : half_dim + 1])
    ml_part[2:8, :] = jnp.zeros((6, n_rows), f32)
    seq_push(3, ml_part, ml_slots)
    seq_push(4, acc_part, acc_slots)

    for k in near_order:
        seq_wait(2, k, kv_part, kv_slots)

    def joined_kv(cols):
        total = kv_part[:, cols].astype(f32)
        for k in near_order:
            total = total + kv_slots[k, :, cols].astype(f32)
        return total * inv_rms

    new_scores = []
    new_values = []
    for h in range(kv_local):
        key = rotate(joined_kv(slice(h * head_dim, (h + 1) * head_dim)), cosine, sine_signed)
        key = key.astype(bf16).astype(f32)
        new_values.append(
            joined_kv(slice(kv_cols + h * head_dim, kv_cols + (h + 1) * head_dim))
            .astype(bf16)
            .astype(f32)
        )
        for g in range(group):
            j = h * group + g
            q = q_rows[j * rows : (j + 1) * rows, :]
            new_scores.append(jnp.sum(q * key, axis=1, keepdims=True) * score_scale)
    score_new = to_lanes(jnp.concatenate(new_scores, axis=0))

    for k in near_order:
        seq_wait(3, k, ml_part, ml_slots)
    stats = [(ml_part[0:1, :], ml_part[1:2, :])]
    stats += [(ml_slots[k, 0:1, :], ml_slots[k, 1:2, :]) for k in near_order]
    row_max = score_new
    for m_one, _ in stats:
        row_max = jnp.maximum(row_max, m_one)
    shares = [jnp.exp(m_one - row_max) * l_one for m_one, l_one in stats]
    new_weight = jnp.exp(score_new - row_max)
    total_weight = new_weight
    for one in shares:
        total_weight = total_weight + one
    factors = [to_rows(one / total_weight) for one in shares]
    new_factor = to_rows(new_weight / total_weight)
    for k in near_order:
        seq_wait(4, k, acc_part, acc_slots)
    for j in range(q_heads):
        at = slice(j * rows, (j + 1) * rows)
        merged = acc_rows[at, :] * factors[0][at] + new_factor[at] * new_values[j // group]
        for i, k in enumerate(near_order):
            merged = merged + acc_slots[k, at, :].astype(f32) * factors[1 + i][at]
        attn_x[:, j * head_dim : (j + 1) * head_dim] = merged.astype(bf16)

    ld_wo.wait()
    x = attn_x[...]
    for n in range(0, feature, tile):
        out_part[:, n : n + tile] = dot(x, wo[:, n : n + tile])
    for k in range(1, head_count):
        copy = pltpu.make_async_remote_copy(
            src_ref=out_part,
            dst_ref=out_slots.at[k],
            send_sem=head_send.at[k],
            recv_sem=head_recv.at[k],
            device_id=peer(0, k),
            device_id_type=MESH,
        )
        copy.start()
        pending.append(copy)
    for k in range(1, head_count):
        pltpu.make_async_remote_copy(
            src_ref=out_part,
            dst_ref=out_slots.at[k],
            send_sem=head_send.at[k],
            recv_sem=head_recv.at[k],
            device_id=peer(0, k),
            device_id_type=MESH,
        ).wait_recv()
    summed = out_part[...]
    for k in range(1, head_count):
        summed = summed + out_slots[k]
    mid = (token_float + summed).astype(bf16)
    mid_part[...] = mid
    seq_push(5, mid_part, mid_slots)

    ld_win.wait()
    ssq_b = jnp.zeros((rows, 1), f32)
    for k in [0] + near_order:
        if k:
            seq_wait(5, k, mid_part, mid_slots)
            block = mid_slots[k].astype(f32)
        else:
            block = mid.astype(f32)
        owner = lax.rem(my_seq - k + seq_count, seq_count)
        ssq_b = ssq_b + jnp.sum(block * block, axis=1, keepdims=True)
        x = (block * gains[owner]).astype(bf16)
        at = pl.ds(pl.multiple_of(owner * feature, feature), feature)
        for i in range(2):
            for n in range(0, chan, tile):
                cols = slice(n, min(n + tile, chan))
                part = dot(x, win[i, at, cols])
                if k:
                    part = part + inner_acc[i, :, cols]
                inner_acc[i, :, cols] = part
    inv_b = lax.rsqrt(ssq_b / model + norm_eps)
    inner = inner_acc[0] * inv_b
    ld_cs.wait()
    taps = conv_weight_ref.shape[0]
    mixed = inner * conv_weight_ref[taps - 1 : taps, :] + conv_bias_ref[...][None, :]
    for k in range(taps - 1):
        mixed = mixed + cs[:, k, :] * conv_weight_ref[k : k + 1, :]
    u = mixed / (1.0 + jnp.exp(-mixed))
    ld_wx.wait()
    proj_width = wx.shape[1]
    proj_part[...] = jnp.zeros(proj_part.shape, f32)
    proj_part[:, :proj_width] = dot(u.astype(bf16), wx[...])
    order = list(enumerate(everyone))

    def all_copy(phase, index, ks, kh, src, slots):
        return pltpu.make_async_remote_copy(
            src_ref=src,
            dst_ref=slots.at[index],
            send_sem=all_send.at[phase, index],
            recv_sem=all_recv.at[phase, index],
            device_id=peer(ks, kh),
            device_id_type=MESH,
        )

    for index, (ks, kh) in order:
        copy = all_copy(0, index, ks, kh, proj_part, proj_slots)
        copy.start()
        pending.append(copy)
    gate = inner_acc[1] * inv_b
    gate_silu = gate / (1.0 + jnp.exp(-gate))
    decay_rate = -jnp.exp(a_log_ref[...])
    ld_wdt.wait()
    ld_state.wait()
    for index, (ks, kh) in order:
        all_copy(0, index, ks, kh, proj_part, proj_slots).wait_recv()
    projected = proj_part[...]
    for index, _ in order:
        projected = projected + proj_slots[index]
    low = dot(projected[:, :rank].astype(bf16), wdt[...]) + dt_bias_ref[...][None, :]
    dt = jnp.maximum(low, 0.0) + jnp.log1p(jnp.exp(-jnp.abs(low)))
    dtu = dt * u
    maps = projected[:, rank:]
    map_lane = lax.broadcasted_iota(jnp.int32, (nstate, maps.shape[1]), 1)
    map_row = lax.broadcasted_iota(jnp.int32, (nstate, maps.shape[1]), 0)
    for b in range(rows):
        line = maps[b : b + 1, :]
        bm = jnp.sum(jnp.where(map_lane == map_row, line, 0.0), axis=1, keepdims=True)
        cm = jnp.sum(jnp.where(map_lane == map_row + nstate, line, 0.0), axis=1, keepdims=True)
        fresh = jnp.exp(dt[b : b + 1, :] * decay_rate) * state[b] + dtu[b : b + 1, :] * bm
        new_state[b] = fresh
        y_rows[b : b + 1, :] = jnp.sum(cm * fresh, axis=0, keepdims=True)
    store = pltpu.make_async_copy(new_state, new_state_hbm, load_sem.at[len(loads)])
    store.start()
    readout = y_rows[...] + skip_gain_ref[...][None, :] * u
    gated_x[...] = (readout * gate_silu).astype(bf16)

    ld_wm.wait()
    own = None
    for ks in seq_order + [0]:
        owner = lax.rem(my_seq + ks, seq_count)
        x = gated_x[...]
        for n in range(0, feature, tile):
            at = pl.ds(pl.multiple_of(owner * feature + n, tile), tile)
            share_part[ks, :, n : n + tile] = dot(x, wm[:, at]).astype(bf16)
        for index, (ps, kh) in order:
            if ps == ks:
                copy = all_copy(1, index, ps, kh, share_part.at[ks], share_slots)
                copy.start()
                pending.append(copy)
    total = share_part[0].astype(f32)
    for index, (ps, kh) in order:
        all_copy(1, index, ps, kh, share_part.at[ps], share_slots).wait_recv()
    for index, _ in order:
        total = total + share_slots[index].astype(f32)
    hidden_ref[...] = (mid_part[...].astype(f32) + total).astype(bf16)
    store.wait()
    for copy in pending:
        copy.wait_send()


def fused(seq_count, head_count, *args):
    (
        tokens,
        attn_gain,
        w_query,
        key_projection_weight,
        value_projection_weight,
        w_attn_out,
        cache_keys,
        stored_value_cache,
        lengths,
        positions,
        mamba_gain,
        w_in,
        conv_weight,
        conv_bias,
        conv_state,
        w_xproj,
        w_dt,
        dt_bias,
        a_log,
        skip_gain,
        ssm_state,
        w_mamba_out,
    ) = args
    rows, feature = tokens.shape
    q_cols = w_query.shape[1]
    kv_cols = key_projection_weight.shape[1]
    head_dim = cache_keys.shape[3]
    kv_local = cache_keys.shape[1]
    ctx = cache_keys.shape[2]
    q_heads = q_cols // head_dim
    chan = w_mamba_out.shape[0]
    n_rows = q_heads * rows
    pair_rows = 2 * q_heads // kv_local
    blocks = n_rows // pair_rows
    proj_pad = -(-w_xproj.shape[1] // 128) * 128
    others = seq_count * head_count - 1
    f32 = jnp.float32
    bf16 = jnp.bfloat16
    big = (
        w_query,
        key_projection_weight,
        value_projection_weight,
        w_attn_out,
        cache_keys,
        stored_value_cache,
        w_in,
        conv_state,
        w_xproj,
        w_dt,
        ssm_state,
        w_mamba_out,
    )
    small = (tokens, attn_gain, mamba_gain, conv_weight, conv_bias, dt_bias, a_log, skip_gain)
    V = pltpu.VMEM
    dma = pltpu.SemaphoreType.DMA
    scratch = [V(a.shape, a.dtype) for a in big] + [
        V(ssm_state.shape, f32),
        dma((len(big) + 1,)),
        V((rows, q_cols), bf16),
        V((rows, 2 * kv_cols), bf16),
        V((rows, head_dim), f32),
        V((seq_count, rows, q_cols), bf16),
        V((seq_count, rows, 2 * kv_cols), bf16),
        V((seq_count, rows, head_dim), f32),
        V((n_rows, head_dim), f32),
        V((blocks, pair_rows, ctx), f32),
        V((n_rows, head_dim), f32),
        V((n_rows, head_dim), f32),
        V((n_rows, head_dim), bf16),
        V((8, n_rows), f32),
        V((seq_count, n_rows, head_dim), bf16),
        V((seq_count, 8, n_rows), f32),
        V((rows, q_cols), bf16),
        V((rows, feature), f32),
        V((head_count, rows, feature), f32),
        V((rows, feature), bf16),
        V((seq_count, rows, feature), bf16),
        V((seq_count, rows, feature), f32),
        V((2, rows, chan), f32),
        V((rows, proj_pad), f32),
        V((others, rows, proj_pad), f32),
        V((rows, chan), f32),
        V((rows, chan), bf16),
        V((seq_count, rows, feature), bf16),
        V((others, rows, feature), bf16),
        dma((6, seq_count)),
        dma((6, seq_count)),
        dma((head_count,)),
        dma((head_count,)),
        dma((2, others)),
        dma((2, others)),
    ]
    smem = pl.BlockSpec(memory_space=pltpu.SMEM)
    vmem = pl.BlockSpec(memory_space=pltpu.VMEM)
    hbm = pl.BlockSpec(memory_space=pl.ANY)
    return pl.pallas_call(
        functools.partial(fused_kernel, seq_count, head_count),
        out_shape=(
            jax.ShapeDtypeStruct((rows, feature), bf16),
            jax.ShapeDtypeStruct(ssm_state.shape, f32),
        ),
        in_specs=[smem, smem] + [vmem] * len(small) + [hbm] * len(big),
        out_specs=(vmem, hbm),
        scratch_shapes=scratch,
        compiler_params=pltpu.CompilerParams(
            collective_id=0, has_side_effects=True, vmem_limit_bytes=60 * 1024 * 1024
        ),
    )(lengths, positions, *small, *big)


def fits(mesh, args):
    tokens, w_query, cache_keys, w_in = args[0], args[2], args[6], args[11]
    seq_count, head_count = mesh.shape["seq"], mesh.shape["head"]
    rows = tokens.shape[0] // (mesh.shape["rep"] * mesh.shape["sub"])
    kv_local = cache_keys.shape[1] // head_count
    group = w_query.shape[1] // (cache_keys.shape[1] * cache_keys.shape[3])
    return (
        rows == 8
        and kv_local % 2 == 0
        and group == 4
        and kv_local * group * rows == 128
        and cache_keys.shape[3] == 128
        and tokens.shape[1] // seq_count % 512 == 0
        and w_in.shape[2] // (seq_count * head_count) % 512 == 0
    )


def solution(mesh):
    in_specs = (
        P(("rep", "sub"), "seq"),
        P("seq"),
        P("seq", "head"),
        P("seq", "head"),
        P("seq", "head"),
        P("head", "seq"),
        P(("rep", "sub"), "head", "seq", None),
        P(("rep", "sub"), "head", "seq", None),
        P(("rep", "sub")),
        P(("rep", "sub")),
        P(),
        P(None, None, ("seq", "head")),
        P(None, ("seq", "head")),
        P(("seq", "head")),
        P(("rep", "sub"), None, ("seq", "head")),
        P(("seq", "head"), None),
        P(None, ("seq", "head")),
        P(("seq", "head")),
        P(None, ("seq", "head")),
        P(("seq", "head")),
        P(("rep", "sub"), None, ("seq", "head")),
        P(("seq", "head"), None),
    )
    out_specs = (P(("rep", "sub"), "seq"), P(("rep", "sub"), None, ("seq", "head")))

    def run(*args):
        body = local
        if fits(mesh, args):
            body = functools.partial(fused, mesh.shape["seq"], mesh.shape["head"])
        return jax.shard_map(
            body, mesh=mesh, in_specs=in_specs, out_specs=out_specs, check_vma=False
        )(*args)

    return run
```

```python
import functools
import math

import jax
import jax.numpy as jnp
from jax import lax
from jax.experimental import pallas as pl
from jax.experimental.pallas import tpu as pltpu
from jax.sharding import PartitionSpec as P

norm_eps = 1e-05
masked_floor = -1e30
rope_base = 10000.0


def joined(value, axis, join):
    pieces = jax.tree.map(lambda part: lax.all_gather(part, axis), value)
    head = jax.tree.map(lambda part: part[0], pieces)
    tail = jax.tree.map(lambda part: part[1:], pieces)
    subtotal, _ = lax.scan(lambda subtotal, section: (join(subtotal, section), None), head, tail)
    return subtotal


def apply_rotary(vectors, positions):
    half_dim = vectors.shape[-1] // 2
    frequency = jnp.exp(
        -math.log(rope_base) * 2.0 * jnp.arange(half_dim, dtype=jnp.float32) / (2 * half_dim)
    )
    angles = positions.astype(jnp.float32)[:, None] * frequency[None, :]
    cosine = jnp.cos(angles)[:, None, :]
    sine_part = jnp.sin(angles)[:, None, :]
    first_half = vectors[..., :half_dim]
    second_half = vectors[..., half_dim:]
    return jnp.concatenate(
        [
            first_half * cosine - second_half * sine_part,
            second_half * cosine + first_half * sine_part,
        ],
        axis=-1,
    )


def join_partial(earlier, later):
    max_one, sum_one, acc_one = earlier
    max_two, sum_two, acc_two = later
    joined_max = jnp.maximum(max_one, max_two)
    factor_one = jnp.exp(max_one - joined_max)
    factor_two = jnp.exp(max_two - joined_max)
    return (
        joined_max,
        sum_one * factor_one + sum_two * factor_two,
        acc_one * factor_one[..., None] + acc_two * factor_two[..., None],
    )


def local(
    tokens,
    attn_gain,
    w_query,
    key_projection_weight,
    value_projection_weight,
    w_attn_out,
    cache_keys,
    stored_value_cache,
    lengths,
    positions,
    mamba_gain,
    w_in,
    conv_weight,
    conv_bias,
    conv_state,
    w_xproj,
    w_dt,
    dt_bias,
    a_log,
    skip_gain,
    ssm_state,
    w_mamba_out,
):
    batch_rows = tokens.shape[0]
    feature_cols = tokens.shape[1]
    head_dim = cache_keys.shape[3]
    kv_local = cache_keys.shape[1]
    ctx_local = cache_keys.shape[2]
    q_local = w_query.shape[1] // head_dim
    query_group_count = q_local // kv_local
    model_width = feature_cols * lax.axis_size("seq")
    token_float = tokens.astype(jnp.float32)
    lifted = (token_float * attn_gain[None, :]).astype(jnp.bfloat16)
    part_query = jnp.dot(lifted, w_query, preferred_element_type=jnp.float32)
    part_key = jnp.dot(lifted, key_projection_weight, preferred_element_type=jnp.float32)
    part_value = jnp.dot(lifted, value_projection_weight, preferred_element_type=jnp.float32)
    squares = jnp.sum(token_float * token_float, axis=1)
    sum_squares = lax.psum(squares, "seq")
    part_query, part_key, part_value = lax.psum((part_query, part_key, part_value), "seq")
    inv_rms = lax.rsqrt(sum_squares / model_width + norm_eps)
    query_vectors = apply_rotary(
        (part_query * inv_rms[:, None]).reshape(batch_rows, q_local, head_dim), positions
    ).astype(jnp.bfloat16)
    fresh_key_rows = apply_rotary(
        (part_key * inv_rms[:, None]).reshape(batch_rows, kv_local, head_dim), positions
    ).astype(jnp.bfloat16)
    fresh_value_rows = (
        (part_value * inv_rms[:, None]).reshape(batch_rows, kv_local, head_dim).astype(jnp.bfloat16)
    )
    grouped_queries = query_vectors.reshape(batch_rows, kv_local, query_group_count, head_dim)
    score_scale = head_dim ** (-0.5)
    scores = (
        jnp.einsum(
            "bhgd,bhtd->bhgt", grouped_queries, cache_keys, preferred_element_type=jnp.float32
        )
        * score_scale
    )
    slot_index = lax.axis_index("seq") * ctx_local + jnp.arange(ctx_local, dtype=jnp.int32)
    live_mask = slot_index[None, None, None, :] < lengths[:, None, None, None]
    local_max = jnp.max(jnp.where(live_mask, scores, masked_floor), axis=-1)
    weights = jnp.where(live_mask, jnp.exp(scores - local_max[..., None]), 0.0)
    local_sum = jnp.sum(weights, axis=-1)
    local_acc = jnp.einsum(
        "bhgt,bhtd->bhgd",
        weights.astype(jnp.bfloat16),
        stored_value_cache,
        preferred_element_type=jnp.float32,
    )
    merged_max, merged_sum, merged_acc = joined(
        (local_max, local_sum, local_acc), "seq", join_partial
    )
    score_new = (
        jnp.einsum(
            "bhgd,bhd->bhg", grouped_queries.astype(jnp.float32), fresh_key_rows.astype(jnp.float32)
        )
        * score_scale
    )
    row_max = jnp.maximum(merged_max, score_new)
    old_factor = jnp.exp(merged_max - row_max)
    new_weight = jnp.exp(score_new - row_max)
    total_weight = merged_sum * old_factor + new_weight
    attended = (
        merged_acc * old_factor[..., None]
        + new_weight[..., None] * fresh_value_rows.astype(jnp.float32)[:, :, None, :]
    )
    attn_rows = (
        (attended / total_weight[..., None])
        .reshape(batch_rows, q_local * head_dim)
        .astype(jnp.bfloat16)
    )
    out_part = jnp.dot(attn_rows, w_attn_out, preferred_element_type=jnp.float32)
    summed = lax.psum(out_part, "head")
    mid_stream = (token_float + summed).astype(jnp.bfloat16)
    full_tokens = lax.all_gather(mid_stream, "seq", axis=1, tiled=True)
    full_float = full_tokens.astype(jnp.float32)
    inv_rms_two = lax.rsqrt(jnp.mean(full_float * full_float, axis=1) + norm_eps)
    lifted_two = (full_float * inv_rms_two[:, None] * mamba_gain[None, :]).astype(jnp.bfloat16)
    inner = jnp.dot(lifted_two, w_in[0], preferred_element_type=jnp.float32)
    gate_branch = jnp.dot(lifted_two, w_in[1], preferred_element_type=jnp.float32)
    window = jnp.concatenate([conv_state, inner[:, None, :]], axis=1)
    mixed = jnp.sum(window * conv_weight[None, :, :], axis=1) + conv_bias[None, :]
    activated = jax.nn.silu(mixed)
    proj_part = jnp.dot(activated.astype(jnp.bfloat16), w_xproj, preferred_element_type=jnp.float32)
    projected = lax.psum(proj_part, ("seq", "head"))
    rank_width = w_dt.shape[0]
    state_width = ssm_state.shape[1]
    dt_low = projected[:, :rank_width].astype(jnp.bfloat16)
    input_map = projected[:, rank_width : rank_width + state_width]
    output_map = projected[:, rank_width + state_width :]
    step_size = jax.nn.softplus(
        jnp.dot(dt_low, w_dt, preferred_element_type=jnp.float32) + dt_bias[None, :]
    )
    decay = jnp.exp(step_size[:, None, :] * (-jnp.exp(a_log))[None, :, :])
    new_state = decay * ssm_state + (step_size * activated)[:, None, :] * input_map[:, :, None]
    readout = jnp.sum(output_map[:, :, None] * new_state, axis=1) + skip_gain[None, :] * activated
    gated = (readout * jax.nn.silu(gate_branch)).astype(jnp.bfloat16)
    mamba_part = jnp.dot(gated, w_mamba_out, preferred_element_type=jnp.float32)
    share = lax.psum_scatter(
        mamba_part.astype(jnp.bfloat16), "seq", scatter_dimension=1, tiled=True
    ).astype(jnp.float32)
    share = lax.psum(share, "head")
    hidden_out = (mid_stream.astype(jnp.float32) + share).astype(jnp.bfloat16)
    return (hidden_out, new_state)


MESH = pl.DeviceIdType.MESH


def farthest_first(count):
    return sorted(range(1, count), key=lambda k: -min(k, count - k))


def rotate(vectors, cosine, sine_signed):
    half_dim = vectors.shape[-1] // 2
    return vectors * cosine + pltpu.roll(vectors, half_dim, 1) * sine_signed


def fused_kernel(
    seq_count,
    head_count,
    length_ref,
    position_ref,
    token_ref,
    attn_gain_ref,
    mamba_gain_ref,
    conv_weight_ref,
    conv_bias_ref,
    dt_bias_ref,
    a_log_ref,
    skip_gain_ref,
    wq_hbm,
    wk_hbm,
    wv_hbm,
    wo_hbm,
    ck_hbm,
    cv_hbm,
    win_hbm,
    cs_hbm,
    wx_hbm,
    wdt_hbm,
    state_hbm,
    wm_hbm,
    hidden_ref,
    new_state_hbm,
    wq,
    wk,
    wv,
    wo,
    ck,
    cv,
    win,
    cs,
    wx,
    wdt,
    state,
    wm,
    new_state,
    load_sem,
    q_part,
    kv_part,
    ssq_part,
    q_slots,
    kv_slots,
    ssq_slots,
    q_rows,
    scores,
    acc_rows,
    ml_rows,
    acc_part,
    ml_part,
    acc_slots,
    ml_slots,
    attn_x,
    out_part,
    out_slots,
    mid_part,
    mid_slots,
    gains,
    inner_acc,
    proj_part,
    proj_slots,
    y_rows,
    gated_x,
    share_part,
    share_slots,
    seq_send,
    seq_recv,
    head_send,
    head_recv,
    all_send,
    all_recv,
):
    rows, feature = token_ref.shape
    head_dim = ck.shape[3]
    kv_local = ck.shape[1]
    ctx = ck.shape[2]
    q_cols = wq.shape[1]
    kv_cols = wk.shape[1]
    q_heads = q_cols // head_dim
    group = q_heads // kv_local
    model = feature * seq_count
    chan = wm.shape[0]
    nstate = a_log_ref.shape[0]
    rank = wdt.shape[0]
    f32 = jnp.float32
    bf16 = jnp.bfloat16
    my_seq = lax.axis_index("seq")
    my_head = lax.axis_index("head")

    def peer(ks, kh):
        return {
            "seq": lax.rem(my_seq + ks, seq_count),
            "head": lax.rem(my_head + kh, head_count),
        }

    loads = []
    for src, dst in (
        (wq_hbm, wq),
        (wk_hbm, wk),
        (wv_hbm, wv),
        (ck_hbm, ck),
        (cv_hbm, cv),
        (wo_hbm, wo),
        (win_hbm, win),
        (cs_hbm, cs),
        (wx_hbm, wx),
        (wdt_hbm, wdt),
        (state_hbm, state),
        (wm_hbm, wm),
    ):
        copy = pltpu.make_async_copy(src, dst, load_sem.at[len(loads)])
        copy.start()
        loads.append(copy)
    (ld_wq, ld_wk, ld_wv, ld_ck, ld_cv, ld_wo, ld_win, ld_cs, ld_wx, ld_wdt, ld_state, ld_wm) = loads

    barrier = pltpu.get_barrier_semaphore()
    everyone = [
        (ks, kh) for ks in range(seq_count) for kh in range(head_count) if ks or kh
    ]
    everyone.sort(key=lambda o: -(min(o[0], seq_count - o[0]) + min(o[1], head_count - o[1])))
    for ks, kh in everyone:
        pl.semaphore_signal(barrier, inc=1, device_id=peer(ks, kh), device_id_type=MESH)

    seq_order = farthest_first(seq_count)
    near_order = seq_order[::-1]
    pending = []

    def seq_push(phase, src, slots):
        for k in seq_order:
            copy = pltpu.make_async_remote_copy(
                src_ref=src,
                dst_ref=slots.at[k],
                send_sem=seq_send.at[phase, k],
                recv_sem=seq_recv.at[phase, k],
                device_id=peer(k, 0),
                device_id_type=MESH,
            )
            copy.start()
            pending.append(copy)

    def seq_wait(phase, k, src, slots):
        pltpu.make_async_remote_copy(
            src_ref=src,
            dst_ref=slots.at[k],
            send_sem=seq_send.at[phase, k],
            recv_sem=seq_recv.at[phase, k],
            device_id=peer(k, 0),
            device_id_type=MESH,
        ).wait_recv()

    token_float = token_ref[...].astype(f32)
    lifted = (token_float * attn_gain_ref[...][None, :]).astype(bf16)
    squares = jnp.sum(token_float * token_float, axis=1, keepdims=True)
    ssq_part[...] = jnp.broadcast_to(squares, ssq_part.shape)

    half_dim = head_dim // 2
    lane = lax.broadcasted_iota(jnp.int32, (rows, head_dim), 1)
    frequency = jnp.exp(
        -math.log(rope_base) * 2.0 * (lane % half_dim).astype(f32) / (2 * half_dim)
    )
    row_index = lax.broadcasted_iota(jnp.int32, (rows, head_dim), 0)
    position = jnp.zeros((rows, head_dim), f32)
    for b in range(rows):
        position = jnp.where(row_index == b, position_ref[b].astype(f32), position)
    angles = position * frequency
    cosine = jnp.cos(angles)
    sine_signed = jnp.where(lane < half_dim, -jnp.sin(angles), jnp.sin(angles))
    mg = mamba_gain_ref[...]
    for s in range(seq_count):
        gains[s] = jnp.broadcast_to(mg[s * feature : (s + 1) * feature][None, :], (rows, feature))

    tile = 512

    def dot(a, b):
        return jnp.dot(a, b, preferred_element_type=f32)

    ld_wq.wait()
    for n in range(0, q_cols, tile):
        q_part[:, n : n + tile] = dot(lifted, wq[:, n : n + tile]).astype(bf16)
    pl.semaphore_wait(barrier, len(everyone))
    seq_push(0, ssq_part, ssq_slots)
    seq_push(1, q_part, q_slots)
    ld_wk.wait()
    kv_part[:, :kv_cols] = dot(lifted, wk[...]).astype(bf16)
    ld_wv.wait()
    kv_part[:, kv_cols:] = dot(lifted, wv[...]).astype(bf16)
    seq_push(2, kv_part, kv_slots)

    for k in near_order:
        seq_wait(0, k, ssq_part, ssq_slots)
        seq_wait(1, k, q_part, q_slots)
    ssq = ssq_part[...]
    for k in near_order:
        ssq = ssq + ssq_slots[k]
    inv_rms = lax.rsqrt(ssq / model + norm_eps)
    for j in range(q_heads):
        cols = slice(j * head_dim, (j + 1) * head_dim)
        total = q_part[:, cols].astype(f32)
        for k in near_order:
            total = total + q_slots[k, :, cols].astype(f32)
        spun = rotate(total * inv_rms, cosine, sine_signed)
        q_rows[j * rows : (j + 1) * rows, :] = spun.astype(bf16).astype(f32)

    score_scale = head_dim ** (-0.5)
    pair_rows = 2 * group
    pair_stride = pair_rows * rows
    upper = lax.broadcasted_iota(jnp.int32, (pair_rows, head_dim), 0) < group
    slot_index = my_seq * ctx + lax.broadcasted_iota(jnp.int32, (pair_rows, ctx), 1)
    pairs = [(b, p) for b in range(rows) for p in range(kv_local // 2)]
    ld_ck.wait()
    for index, (b, p) in enumerate(pairs):
        x = q_rows[pl.ds(p * pair_stride + b, pair_rows, stride=rows), :]
        left = jnp.concatenate([jnp.where(upper, x, 0.0), jnp.where(upper, 0.0, x)], axis=1)
        keys = jnp.concatenate([ck[b, 2 * p], ck[b, 2 * p + 1]], axis=1)
        scores[index] = lax.dot_general(
            left.astype(bf16), keys, (((1,), (1,)), ((), ())), preferred_element_type=f32
        )
    ld_cv.wait()
    lane_row = lax.broadcasted_iota(jnp.int32, (pair_rows, head_dim), 1)
    for index, (b, p) in enumerate(pairs):
        live = slot_index < length_ref[b]
        s = jnp.where(live, scores[index] * score_scale, masked_floor)
        top = jnp.max(s, axis=1, keepdims=True)
        w = jnp.where(live, jnp.exp(s - top), 0.0)
        sum_w = jnp.sum(w, axis=1, keepdims=True)
        values = jnp.concatenate([cv[b, 2 * p], cv[b, 2 * p + 1]], axis=1)
        both = dot(w.astype(bf16), values)
        acc = jnp.where(upper, both[:, :head_dim], both[:, head_dim:])
        acc = acc / jnp.maximum(sum_w, 1e-30)
        spot = pl.ds(p * pair_stride + b, pair_rows, stride=rows)
        acc_rows[spot, :] = acc
        ml_rows[spot, :] = jnp.where(lane_row < half_dim, top, sum_w)
    acc_part[...] = acc_rows[...].astype(bf16)
    n_rows = q_heads * rows
    diag = lax.broadcasted_iota(jnp.int32, (n_rows, n_rows), 0) == lax.broadcasted_iota(
        jnp.int32, (n_rows, n_rows), 1
    )

    def to_lanes(column):
        return jnp.sum(jnp.where(diag, column, 0.0), axis=0, keepdims=True)

    def to_rows(line):
        return jnp.sum(jnp.where(diag, line, 0.0), axis=1, keepdims=True)

    ml = ml_rows[...]
    ml_part[0:1, :] = to_lanes(ml[:, 0:1])
    ml_part[1:2, :] = to_lanes(ml[:, half_dim : half_dim + 1])
    ml_part[2:8, :] = jnp.zeros((6, n_rows), f32)
    seq_push(3, ml_part, ml_slots)
    seq_push(4, acc_part, acc_slots)

    for k in near_order:
        seq_wait(2, k, kv_part, kv_slots)

    def joined_kv(cols):
        total = kv_part[:, cols].astype(f32)
        for k in near_order:
            total = total + kv_slots[k, :, cols].astype(f32)
        return total * inv_rms

    new_scores = []
    new_values = []
    for h in range(kv_local):
        key = rotate(joined_kv(slice(h * head_dim, (h + 1) * head_dim)), cosine, sine_signed)
        key = key.astype(bf16).astype(f32)
        new_values.append(
            joined_kv(slice(kv_cols + h * head_dim, kv_cols + (h + 1) * head_dim))
            .astype(bf16)
            .astype(f32)
        )
        for g in range(group):
            j = h * group + g
            q = q_rows[j * rows : (j + 1) * rows, :]
            new_scores.append(jnp.sum(q * key, axis=1, keepdims=True) * score_scale)
    score_new = to_lanes(jnp.concatenate(new_scores, axis=0))

    for k in near_order:
        seq_wait(3, k, ml_part, ml_slots)
    stats = [(ml_part[0:1, :], ml_part[1:2, :])]
    stats += [(ml_slots[k, 0:1, :], ml_slots[k, 1:2, :]) for k in near_order]
    row_max = score_new
    for m_one, _ in stats:
        row_max = jnp.maximum(row_max, m_one)
    shares = [jnp.exp(m_one - row_max) * l_one for m_one, l_one in stats]
    new_weight = jnp.exp(score_new - row_max)
    total_weight = new_weight
    for one in shares:
        total_weight = total_weight + one
    factors = [to_rows(one / total_weight) for one in shares]
    new_factor = to_rows(new_weight / total_weight)
    for k in near_order:
        seq_wait(4, k, acc_part, acc_slots)
    for j in range(q_heads):
        at = slice(j * rows, (j + 1) * rows)
        merged = acc_rows[at, :] * factors[0][at] + new_factor[at] * new_values[j // group]
        for i, k in enumerate(near_order):
            merged = merged + acc_slots[k, at, :].astype(f32) * factors[1 + i][at]
        attn_x[:, j * head_dim : (j + 1) * head_dim] = merged.astype(bf16)

    ld_wo.wait()
    x = attn_x[...]
    for n in range(0, feature, tile):
        out_part[:, n : n + tile] = dot(x, wo[:, n : n + tile])
    for k in range(1, head_count):
        copy = pltpu.make_async_remote_copy(
            src_ref=out_part,
            dst_ref=out_slots.at[k],
            send_sem=head_send.at[k],
            recv_sem=head_recv.at[k],
            device_id=peer(0, k),
            device_id_type=MESH,
        )
        copy.start()
        pending.append(copy)
    for k in range(1, head_count):
        pltpu.make_async_remote_copy(
            src_ref=out_part,
            dst_ref=out_slots.at[k],
            send_sem=head_send.at[k],
            recv_sem=head_recv.at[k],
            device_id=peer(0, k),
            device_id_type=MESH,
        ).wait_recv()
    summed = out_part[...]
    for k in range(1, head_count):
        summed = summed + out_slots[k]
    mid = (token_float + summed).astype(bf16)
    mid_part[...] = mid
    seq_push(5, mid_part, mid_slots)

    ld_win.wait()
    ssq_b = jnp.zeros((rows, 1), f32)
    for k in [0] + near_order:
        if k:
            seq_wait(5, k, mid_part, mid_slots)
            block = mid_slots[k].astype(f32)
        else:
            block = mid.astype(f32)
        owner = lax.rem(my_seq - k + seq_count, seq_count)
        ssq_b = ssq_b + jnp.sum(block * block, axis=1, keepdims=True)
        x = (block * gains[owner]).astype(bf16)
        at = pl.ds(pl.multiple_of(owner * feature, feature), feature)
        for i in range(2):
            for n in range(0, chan, tile):
                cols = slice(n, min(n + tile, chan))
                part = dot(x, win[i, at, cols])
                if k:
                    part = part + inner_acc[i, :, cols]
                inner_acc[i, :, cols] = part
    inv_b = lax.rsqrt(ssq_b / model + norm_eps)
    inner = inner_acc[0] * inv_b
    ld_cs.wait()
    taps = conv_weight_ref.shape[0]
    mixed = inner * conv_weight_ref[taps - 1 : taps, :] + conv_bias_ref[...][None, :]
    for k in range(taps - 1):
        mixed = mixed + cs[k] * conv_weight_ref[k : k + 1, :]
    u = mixed / (1.0 + jnp.exp(-mixed))
    ld_wx.wait()
    proj_width = wx.shape[0]
    proj_part[...] = jnp.zeros(proj_part.shape, bf16)
    proj_part[:, :proj_width] = lax.dot_general(
        u.astype(bf16), wx[...], (((1,), (1,)), ((), ())), preferred_element_type=f32
    ).astype(bf16)
    order = list(enumerate(everyone))

    def all_copy(phase, index, ks, kh, src, slots):
        return pltpu.make_async_remote_copy(
            src_ref=src,
            dst_ref=slots.at[index],
            send_sem=all_send.at[phase, index],
            recv_sem=all_recv.at[phase, index],
            device_id=peer(ks, kh),
            device_id_type=MESH,
        )

    for index, (ks, kh) in order:
        copy = all_copy(0, index, ks, kh, proj_part, proj_slots)
        copy.start()
        pending.append(copy)
    gate = inner_acc[1] * inv_b
    gate_silu = gate / (1.0 + jnp.exp(-gate))
    decay_rate = -jnp.exp(a_log_ref[...])
    ld_wdt.wait()
    ld_state.wait()
    for index, (ks, kh) in order:
        all_copy(0, index, ks, kh, proj_part, proj_slots).wait_recv()
    projected = proj_part[...].astype(f32)
    for index, _ in order:
        projected = projected + proj_slots[index].astype(f32)
    low = dot(projected[:, :rank].astype(bf16), wdt[...]) + dt_bias_ref[...][None, :]
    dt = jnp.maximum(low, 0.0) + jnp.log1p(jnp.exp(-jnp.abs(low)))
    dtu = dt * u
    maps = projected[:, rank:]
    map_lane = lax.broadcasted_iota(jnp.int32, (nstate, maps.shape[1]), 1)
    map_row = lax.broadcasted_iota(jnp.int32, (nstate, maps.shape[1]), 0)
    for b in range(rows):
        line = maps[b : b + 1, :]
        bm = jnp.sum(jnp.where(map_lane == map_row, line, 0.0), axis=1, keepdims=True)
        cm = jnp.sum(jnp.where(map_lane == map_row + nstate, line, 0.0), axis=1, keepdims=True)
        fresh = jnp.exp(dt[b : b + 1, :] * decay_rate) * state[b] + dtu[b : b + 1, :] * bm
        new_state[b] = fresh
        y_rows[b : b + 1, :] = jnp.sum(cm * fresh, axis=0, keepdims=True)
    store = pltpu.make_async_copy(new_state, new_state_hbm, load_sem.at[len(loads)])
    store.start()
    readout = y_rows[...] + skip_gain_ref[...][None, :] * u
    gated_x[...] = (readout * gate_silu).astype(bf16)

    ld_wm.wait()
    own = None
    for ks in seq_order + [0]:
        owner = lax.rem(my_seq + ks, seq_count)
        x = gated_x[...]
        for n in range(0, feature, tile):
            at = pl.ds(pl.multiple_of(owner * feature + n, tile), tile)
            share_part[ks, :, n : n + tile] = dot(x, wm[:, at]).astype(bf16)
        for index, (ps, kh) in order:
            if ps == ks:
                copy = all_copy(1, index, ps, kh, share_part.at[ks], share_slots)
                copy.start()
                pending.append(copy)
    total = share_part[0].astype(f32)
    for index, (ps, kh) in order:
        all_copy(1, index, ps, kh, share_part.at[ps], share_slots).wait_recv()
    for index, _ in order:
        total = total + share_slots[index].astype(f32)
    hidden_ref[...] = (mid_part[...].astype(f32) + total).astype(bf16)
    store.wait()
    for copy in pending:
        copy.wait_send()


def fused(seq_count, head_count, *args):
    (
        tokens,
        attn_gain,
        w_query,
        key_projection_weight,
        value_projection_weight,
        w_attn_out,
        cache_keys,
        stored_value_cache,
        lengths,
        positions,
        mamba_gain,
        w_in,
        conv_weight,
        conv_bias,
        conv_state,
        w_xproj,
        w_dt,
        dt_bias,
        a_log,
        skip_gain,
        ssm_state,
        w_mamba_out,
    ) = args
    rows, feature = tokens.shape
    q_cols = w_query.shape[1]
    kv_cols = key_projection_weight.shape[1]
    head_dim = cache_keys.shape[3]
    kv_local = cache_keys.shape[1]
    ctx = cache_keys.shape[2]
    q_heads = q_cols // head_dim
    chan = w_mamba_out.shape[0]
    n_rows = q_heads * rows
    pair_rows = 2 * q_heads // kv_local
    blocks = n_rows // pair_rows
    proj_pad = -(-w_xproj.shape[1] // 128) * 128
    others = seq_count * head_count - 1
    f32 = jnp.float32
    bf16 = jnp.bfloat16
    conv_state = jnp.transpose(conv_state, (1, 0, 2))
    w_xproj = w_xproj.T
    big = (
        w_query,
        key_projection_weight,
        value_projection_weight,
        w_attn_out,
        cache_keys,
        stored_value_cache,
        w_in,
        conv_state,
        w_xproj,
        w_dt,
        ssm_state,
        w_mamba_out,
    )
    small = (tokens, attn_gain, mamba_gain, conv_weight, conv_bias, dt_bias, a_log, skip_gain)
    V = pltpu.VMEM
    dma = pltpu.SemaphoreType.DMA
    scratch = [V(a.shape, a.dtype) for a in big] + [
        V(ssm_state.shape, f32),
        dma((len(big) + 1,)),
        V((rows, q_cols), bf16),
        V((rows, 2 * kv_cols), bf16),
        V((rows, head_dim), f32),
        V((seq_count, rows, q_cols), bf16),
        V((seq_count, rows, 2 * kv_cols), bf16),
        V((seq_count, rows, head_dim), f32),
        V((n_rows, head_dim), f32),
        V((blocks, pair_rows, ctx), f32),
        V((n_rows, head_dim), f32),
        V((n_rows, head_dim), f32),
        V((n_rows, head_dim), bf16),
        V((8, n_rows), f32),
        V((seq_count, n_rows, head_dim), bf16),
        V((seq_count, 8, n_rows), f32),
        V((rows, q_cols), bf16),
        V((rows, feature), f32),
        V((head_count, rows, feature), f32),
        V((rows, feature), bf16),
        V((seq_count, rows, feature), bf16),
        V((seq_count, rows, feature), f32),
        V((2, rows, chan), f32),
        V((rows, proj_pad), bf16),
        V((others, rows, proj_pad), bf16),
        V((rows, chan), f32),
        V((rows, chan), bf16),
        V((seq_count, rows, feature), bf16),
        V((others, rows, feature), bf16),
        dma((6, seq_count)),
        dma((6, seq_count)),
        dma((head_count,)),
        dma((head_count,)),
        dma((2, others)),
        dma((2, others)),
    ]
    smem = pl.BlockSpec(memory_space=pltpu.SMEM)
    vmem = pl.BlockSpec(memory_space=pltpu.VMEM)
    hbm = pl.BlockSpec(memory_space=pl.ANY)
    return pl.pallas_call(
        functools.partial(fused_kernel, seq_count, head_count),
        out_shape=(
            jax.ShapeDtypeStruct((rows, feature), bf16),
            jax.ShapeDtypeStruct(ssm_state.shape, f32),
        ),
        in_specs=[smem, smem] + [vmem] * len(small) + [hbm] * len(big),
        out_specs=(vmem, hbm),
        scratch_shapes=scratch,
        compiler_params=pltpu.CompilerParams(
            collective_id=0, has_side_effects=True, vmem_limit_bytes=60 * 1024 * 1024
        ),
    )(lengths, positions, *small, *big)


def fits(mesh, args):
    tokens, w_query, cache_keys, w_in = args[0], args[2], args[6], args[11]
    seq_count, head_count = mesh.shape["seq"], mesh.shape["head"]
    rows = tokens.shape[0] // (mesh.shape["rep"] * mesh.shape["sub"])
    kv_local = cache_keys.shape[1] // head_count
    group = w_query.shape[1] // (cache_keys.shape[1] * cache_keys.shape[3])
    return (
        rows == 8
        and kv_local % 2 == 0
        and group == 4
        and kv_local * group * rows == 128
        and cache_keys.shape[3] == 128
        and tokens.shape[1] // seq_count % 512 == 0
        and w_in.shape[2] // (seq_count * head_count) % 512 == 0
    )


def solution(mesh):
    in_specs = (
        P(("rep", "sub"), "seq"),
        P("seq"),
        P("seq", "head"),
        P("seq", "head"),
        P("seq", "head"),
        P("head", "seq"),
        P(("rep", "sub"), "head", "seq", None),
        P(("rep", "sub"), "head", "seq", None),
        P(("rep", "sub")),
        P(("rep", "sub")),
        P(),
        P(None, None, ("seq", "head")),
        P(None, ("seq", "head")),
        P(("seq", "head")),
        P(("rep", "sub"), None, ("seq", "head")),
        P(("seq", "head"), None),
        P(None, ("seq", "head")),
        P(("seq", "head")),
        P(None, ("seq", "head")),
        P(("seq", "head")),
        P(("rep", "sub"), None, ("seq", "head")),
        P(("seq", "head"), None),
    )
    out_specs = (P(("rep", "sub"), "seq"), P(("rep", "sub"), None, ("seq", "head")))

    def run(*args):
        body = local
        if fits(mesh, args):
            body = functools.partial(fused, mesh.shape["seq"], mesh.shape["head"])
        return jax.shard_map(
            body, mesh=mesh, in_specs=in_specs, out_specs=out_specs, check_vma=False
        )(*args)

    return run
```
